32 devices in a mesh: bx: 4 (over z), by: 2 (over x), bz: 4 (over y, core).
Axes of the slice: x: 2, y: 2, z: 4, core: 2. Of those that a mesh axis runs over, the one named last changes fastest.
Arguments:
- estimate: float32 [64, 32, 512], P('bx', 'by', 'bz'), may hold values from 0.2 to 5
- observed: float32 [8, 64, 32, 512], P(None, 'bx', 'by', 'bz'), may hold values from 0.3 to 180, as said below
- coverage: int32 [8, 4, 2, 4], P(None, 'bx', 'by', 'bz'), may hold values from 0 to 1, as said below
- psf_taps: float32 [8, 3, 17], replicated, may hold values from 0.05 to 1
Outputs:
- refined: float32 [64, 32, 512], P('bx', 'by', 'bz')
The draws below stay inside these ranges and needn't reach their ends.
Inputs may be any that keep to these rules, and one draw needn't show every extreme that they name: `coverage`: each block is covered by 2 to 8 views; in every draw some block is covered by all 8. `observed`: positive.
All inputs are finite; a program needn't handle non-finite values.
Results may differ from the reference program's by a relative error of at most 0.0001.
Values sent between devices are 32-bit elements; how exact they have to be, the bound alone decides.
A program may use at most 64 MiB of HBM per device.

```python
import math
import jax
import jax.numpy as jnp
from jax import lax

V = 8
R = 8
CX = 16
CY = 16
CZ = 128
NX = 64
NY = 32
NZ = 512
N_BX = 4
N_BY = 2
N_BZ = 4


def draw_observed(key, part):
    first, second = jax.random.split(key, 2)
    blocks_x = NX // CX
    blocks_y = NY // CY
    blocks_z = NZ // CZ
    coarse = jnp.exp(jax.random.uniform(first, (blocks_x, blocks_y, blocks_z), jnp.float32, 0.0, jnp.log(10.0)))
    ramp = 1.0 + 2.0 * jnp.arange(blocks_y, dtype=jnp.float32) / max(blocks_y - 1, 1)
    coarse = coarse * ramp[None, :, None]
    grown = jnp.repeat(jnp.repeat(jnp.repeat(coarse, CX, axis=0), CY, axis=1), CZ, axis=2)
    voxel = jnp.exp(jax.random.uniform(second, (V, NX, NY, NZ), jnp.float32, jnp.log(0.3), jnp.log(3.0)))
    values = voxel * grown[None]
    return values.astype(jnp.float32)


def draw_coverage(key, part):
    blocks = NX // CX * (NY // CY) * (NZ // CZ)
    first, second, third = jax.random.split(jax.random.fold_in(key, 7), 3)
    counts = jax.random.randint(first, (blocks,), 2, V + 1)
    fullest = jax.random.randint(second, (), 0, blocks)
    counts = counts.at[fullest].set(V)
    ranks = jax.vmap(lambda each: jax.random.permutation(each, V))(jax.random.split(third, blocks))
    covered = (ranks < counts[:, None]).astype(jnp.int32)
    return covered.T.reshape(V, NX // CX, NY // CY, NZ // CZ)


def levels(key, dims, cuts, least, high):
    def one(position, shards_of):
        steps = jax.random.uniform(jax.random.fold_in(jax.random.fold_in(key, 6), position), (shards_of,), jnp.float32, least / len(cuts), high / len(cuts))
        return jnp.repeat(jnp.exp(steps), dims[position] // shards_of).reshape((-1,) + (1,) * (len(dims) - position - 1))

    factor_of = one(*cuts[0])
    for cut in cuts[1:]:
        factor_of = factor_of * one(*cut)
    return factor_of


def setup_inputs(seed: int = 0) -> dict:
    key_list = jax.random.split(jax.random.key(seed), 5)
    return {
        "estimate": jnp.clip(jnp.exp(math.log(5.0) - 3.218876 * jax.random.uniform(key_list[0], (NX, NY, NZ), jnp.float32) ** levels(key_list[0], (NX, NY, NZ), ((0, 4), (1, 2), (2, 4)), -0.2, 0.2)), 0.2, 5.0),
        "observed": draw_observed(jax.random.fold_in(key_list[4], 71), 0),
        "coverage": draw_coverage(jax.random.fold_in(key_list[4], 71), 0),
        "psf_taps": jnp.clip(jnp.exp(jax.random.uniform(key_list[3], (V, 3, 2 * R + 1), jnp.float32, math.log(0.05), math.log(1.0))), 0.05, 1.0),
    }


def blur_axis(field, taps_row, axis):
    moved = jnp.moveaxis(field, axis, -1)
    shape = moved.shape
    flat = moved.reshape(-1, 1, shape[-1])
    kernel = taps_row.reshape(1, 1, -1)
    width = (taps_row.shape[0] - 1) // 2
    result = lax.conv_general_dilated(flat, kernel, (1,), [(width, width)], precision=lax.Precision.HIGHEST)
    return jnp.moveaxis(result.reshape(shape), -1, axis)


def blur_volume(field, kernels):
    result = field
    for axis in range(3):
        result = blur_axis(result, kernels[axis], axis)
    return result


def spread(block_values):
    grown = jnp.broadcast_to(block_values[:, None, :, None, :, None], (N_BX, CX, N_BY, CY, N_BZ, CZ))
    return grown.reshape(NX, NY, NZ)


def reference(estimate, observed, coverage, psf_taps):
    taps = psf_taps / jnp.sum(psf_taps, axis=2, keepdims=True)
    weights = coverage.astype(jnp.float32)
    count = spread(jnp.sum(weights, axis=0))
    summed = jnp.zeros((NX, NY, NZ), jnp.float32)
    target_field = jnp.zeros((NX, NY, NZ), jnp.float32)
    for view in range(V):
        blurred = blur_volume(estimate, taps[view])
        ratio = observed[view] / blurred
        back = blur_volume(ratio, taps[view][:, ::-1])
        weight_full = spread(weights[view])
        summed = summed + weight_full * back
        target_field = target_field + weight_full * observed[view]
    updated = estimate * (summed / count)
    target = jnp.sum(target_field / count)
    total = jnp.sum(updated)
    return updated * (target / total)
```

```python
import functools

import jax
import jax.numpy as jnp
from jax import lax
from jax.experimental import pallas as pl
from jax.experimental.pallas import tpu as pltpu
from jax.sharding import PartitionSpec as P

F32 = jnp.float32
BF16 = jnp.bfloat16
MESH = pl.DeviceIdType.MESH


def split(values):
    high = values.astype(BF16)
    low = (values - high.astype(F32)).astype(BF16)
    return high, low


def dot3(left, right, dims=((1,), (0,))):
    def one(a, b):
        return lax.dot_general(a, b, (dims, ((), ())), preferred_element_type=F32)

    return one(left[0], right[0]) + (one(left[0], right[1]) + one(left[1], right[0]))


def kernel(
    sizes,
    taps_ref,
    cover_ref,
    est_ref,
    obs_hbm,
    out_ref,
    obs,
    ext,
    ext_hi,
    ext_lo,
    pack,
    from_left,
    from_right,
    weight,
    weight_xy,
    weight_left,
    weight_right,
    scale,
    band_hi,
    band_lo,
    gath_hi,
    gath_lo,
    scat_hi,
    scat_lo,
    lined,
    spread,
    total,
    fringe,
    back_pack,
    back_left,
    back_right,
    back_xy,
    stat,
    stat_a,
    stat_b,
    part_a,
    obs_sem,
    xy_send,
    xy_recv,
    wxy_send,
    wxy_recv,
    z_send,
    z_recv,
    bz_send,
    bz_recv,
    bxy_send,
    bxy_recv,
    a_send,
    a_recv,
    b_send,
    b_recv,
):
    n_x, n_y, n_z = sizes
    views, rows, cols, lanes = obs.shape
    length = taps_ref.shape[2]
    rad = (length - 1) // 2
    wide_x, wide_y = rows + 2 * rad, cols + 2 * rad
    groups = wide_x // 8
    me_x, me_y, me_z = lax.axis_index("bx"), lax.axis_index("by"), lax.axis_index("bz")

    fetch = pltpu.make_async_copy(obs_hbm, obs, obs_sem)
    fetch.start()

    def exists(dx, dy, dz):
        ok = None
        for step, me, count in ((dx, me_x, n_x), (dy, me_y, n_y), (dz, me_z, n_z)):
            if step == 0:
                continue
            inside = (me + step >= 0) & (me + step < count)
            ok = inside if ok is None else ok & inside
        return ok

    def device(dx, dy, dz):
        return {"bx": me_x + dx, "by": me_y + dy, "bz": me_z + dz}

    around = [(dx, dy) for dx in (-1, 0, 1) for dy in (-1, 0, 1) if (dx, dy) != (0, 0)]
    ring_a = [(i, j) for i in range(n_y) for j in range(n_z) if (i, j) != (0, 0)]

    def device_a(i, j):
        return {"bx": me_x, "by": lax.rem(me_y + i, n_y), "bz": lax.rem(me_z + j, n_z)}

    def device_b(i):
        return {"bx": lax.rem(me_x + i, n_x), "by": me_y, "bz": me_z}

    ext[...] = jnp.zeros(ext.shape, F32)
    ext[rad : rad + rows, rad : rad + cols, :] = est_ref[...]
    from_left[...] = jnp.zeros(from_left.shape, F32)
    from_right[...] = jnp.zeros(from_right.shape, F32)
    weight_xy[...] = jnp.zeros(weight_xy.shape, F32)
    weight_left[...] = jnp.zeros(weight_left.shape, F32)
    weight_right[...] = jnp.zeros(weight_right.shape, F32)
    back_xy[...] = jnp.zeros(back_xy.shape, F32)
    back_left[...] = jnp.zeros(back_left.shape, F32)
    back_right[...] = jnp.zeros(back_right.shape, F32)
    for v in range(views):
        row = jnp.full((1, lanes), cover_ref[v], jnp.int32).astype(F32)
        weight[v : v + 1, :] = row
        weight_xy[1, 1, v : v + 1, :] = row

    barrier = pltpu.get_barrier_semaphore()
    expected = len(ring_a) + n_x - 1
    for i, j in ring_a:
        pl.semaphore_signal(barrier, inc=1, device_id=device_a(i, j), device_id_type=MESH)
    for i in range(1, n_x):
        pl.semaphore_signal(barrier, inc=1, device_id=device_b(i), device_id_type=MESH)
    for dx, dy in around:
        if dx != 0 and dy != 0:
            ok = exists(dx, dy, 0)

            @pl.when(ok)
            def _():
                pl.semaphore_signal(barrier, inc=1, device_id=device(dx, dy, 0), device_id_type=MESH)

            expected = expected + ok.astype(jnp.int32)
    pl.semaphore_wait(barrier, expected)

    def cut(step, size):
        return pl.ds(0, size) if step == 0 else (pl.ds(0, rad) if step < 0 else pl.ds(size - rad, rad))

    def wide(step, size):
        return pl.ds(rad, size) if step == 0 else (pl.ds(0, rad) if step < 0 else pl.ds(rad + size, rad))

    def xy_copies():
        for slot, (dx, dy) in enumerate(around):
            copies = [
                pltpu.make_async_remote_copy(
                    src_ref=est_ref.at[cut(dx, rows), cut(dy, cols), :],
                    dst_ref=ext.at[wide(-dx, rows), wide(-dy, cols), :],
                    send_sem=xy_send.at[slot],
                    recv_sem=xy_recv.at[slot],
                    device_id=device(dx, dy, 0),
                    device_id_type=MESH,
                ),
                pltpu.make_async_remote_copy(
                    src_ref=weight,
                    dst_ref=weight_xy.at[1 - dx, 1 - dy],
                    send_sem=wxy_send.at[slot],
                    recv_sem=wxy_recv.at[slot],
                    device_id=device(dx, dy, 0),
                    device_id_type=MESH,
                ),
            ]
            yield exists(dx, dy, 0), exists(-dx, -dy, 0), copies

    def z_copies():
        for slot, (dz, pack_to, weight_to) in enumerate(
            ((-1, from_right, weight_right), (1, from_left, weight_left))
        ):
            copies = [
                pltpu.make_async_remote_copy(
                    src_ref=source,
                    dst_ref=target,
                    send_sem=z_send.at[slot, which],
                    recv_sem=z_recv.at[slot, which],
                    device_id=device(0, 0, dz),
                    device_id_type=MESH,
                )
                for which, (source, target) in enumerate(((pack, pack_to), (weight_xy, weight_to)))
            ]
            yield exists(0, 0, dz), exists(0, 0, -dz), copies

    def back_z_copies():
        for slot, (dz, target) in enumerate(((-1, back_right), (1, back_left))):
            copy = pltpu.make_async_remote_copy(
                src_ref=back_pack,
                dst_ref=target,
                send_sem=bz_send.at[slot],
                recv_sem=bz_recv.at[slot],
                device_id=device(0, 0, dz),
                device_id_type=MESH,
            )
            yield exists(0, 0, dz), exists(0, 0, -dz), [copy]

    def back_xy_copies():
        for slot, (dx, dy) in enumerate(around):
            copy = pltpu.make_async_remote_copy(
                src_ref=total.at[wide(dx, rows), wide(dy, cols), :],
                dst_ref=back_xy.at[wide(-dx, rows), wide(-dy, cols), :],
                send_sem=bxy_send.at[slot],
                recv_sem=bxy_recv.at[slot],
                device_id=device(dx, dy, 0),
                device_id_type=MESH,
            )
            yield exists(dx, dy, 0), exists(-dx, -dy, 0), [copy]

    def start(family):
        for sends, _, copies in family():

            @pl.when(sends)
            def _():
                for copy in copies:
                    copy.start()

    def arrive(family):
        for _, takes, copies in family():

            @pl.when(takes)
            def _():
                for copy in copies:
                    copy.wait_recv()

    def leave(family):
        for sends, _, copies in family():

            @pl.when(sends)
            def _():
                for copy in copies:
                    copy.wait_send()

    start(xy_copies)

    def build(v, carry):
        def summed(dim):
            values = [taps_ref[v, dim, k] for k in range(length)]
            while len(values) > 1:
                values = [sum(values[i : i + 2]) for i in range(0, len(values), 2)]
            return jnp.full((8, lanes), values[0], F32)

        inverse = 1.0 / (summed(0) * summed(1) * summed(2))

        def chosen(offset, dim):
            result = jnp.zeros(offset.shape, F32)
            for k in range(length):
                result = jnp.where(offset == k, taps_ref[v, dim, k], result)
            return result

        def iota(shape, dim):
            return lax.broadcasted_iota(jnp.int32, shape, dim)

        shape = (lanes, lanes)
        main = chosen(iota(shape, 0) - iota(shape, 1) + rad, 2)
        shape = (2 * rad, lanes)
        row, col = iota(shape, 0), iota(shape, 1)
        edge = chosen(jnp.where(row < rad, row, row + lanes) - col, 2)
        for first, part in ((0, main), (lanes, edge)):
            part = (part.reshape(-1, 8, lanes) * inverse[None]).reshape(part.shape)
            high, low = split(part)
            band_hi[v, first : first + part.shape[0], :] = high
            band_lo[v, first : first + part.shape[0], :] = low
        rest = band_hi.shape[1] - lanes - 2 * rad
        band_hi[v, lanes + 2 * rad :, :] = jnp.zeros((rest, lanes), BF16)
        band_lo[v, lanes + 2 * rad :, :] = jnp.zeros((rest, lanes), BF16)
        shape = (8 * cols, 8 * wide_y)
        row, col = iota(shape, 0), iota(shape, 1)
        offset = jnp.where(row // cols == col // wide_y, col % wide_y - row % cols, -1)
        high, low = split(chosen(offset, 1))
        gath_hi[v], gath_lo[v] = high, low
        shape = (8 * wide_y, 8 * cols)
        row, col = iota(shape, 0), iota(shape, 1)
        offset = jnp.where(row // wide_y == col // cols, row % wide_y - col % cols, -1)
        high, low = split(chosen(offset, 1))
        scat_hi[v], scat_lo[v] = high, low
        return carry

    lax.fori_loop(0, views, build, 0)

    fetch.wait()
    count = jnp.zeros((1, lanes), F32)
    seen = jnp.zeros((8, lanes), F32)
    for v in range(views):
        count = count + weight[v : v + 1, :]
        seen = seen + weight[v : v + 1, :] * jnp.sum(obs[v].reshape(-1, 8, lanes), axis=0)
    stat[0] = seen / count

    arrive(xy_copies)
    lane = lax.broadcasted_iota(jnp.int32, (wide_y, lanes), 1)
    for g in range(groups):
        merged = jnp.zeros((wide_y, lanes), F32)
        for i in range(8):
            rolled = pltpu.roll(ext[8 * g + i], 2 * rad * i + rad, 1)
            merged = jnp.where(lane // (2 * rad) == i, rolled, merged)
        pack[g] = merged
    start(z_copies)
    high, low = split(ext[...].reshape(wide_x * wide_y, lanes))
    ext_hi[:, :lanes] = high
    ext_lo[:, :lanes] = low
    arrive(z_copies)
    for g in range(groups):
        merged = jnp.where(lane % (2 * rad) < rad, from_left[g], from_right[g])
        for i in range(8):
            shift = (lanes - 2 * rad * i) % lanes
            rolled = pltpu.roll(merged, shift, 1) if shift else merged
            high, low = split(rolled)
            first = (8 * g + i) * wide_y
            ext_hi[first : first + wide_y, lanes:] = high
            ext_lo[first : first + wide_y, lanes:] = low

    thin = lax.broadcasted_iota(jnp.int32, (rad, lanes), 1)
    for v in range(views):
        for dx in range(3):
            for dy in range(3):
                mid = jnp.broadcast_to(weight_xy[dx, dy, v : v + 1, :], (rad, lanes))
                left = jnp.broadcast_to(weight_left[dx, dy, v : v + 1, :], (rad, lanes))
                right = jnp.broadcast_to(weight_right[dx, dy, v : v + 1, :], (rad, lanes))
                side = jnp.where(thin < rad, left, jnp.where(thin < 2 * rad, right, 0.0))
                for first in range(0 if dy == 0 else (rad if dy == 1 else rad + cols), rad if dy == 0 else (rad + cols if dy == 1 else wide_y), rad):
                    scale[v, dx, first : first + rad, :lanes] = mid
                    scale[v, dx, first : first + rad, lanes:] = side

    total[...] = jnp.zeros(total.shape, F32)
    fringe[...] = jnp.zeros(fringe.shape, F32)

    def one_view(v, carry):
        band = band_hi[v], band_lo[v]
        gath = gath_hi[v], gath_lo[v]
        scat = scat_hi[v], scat_lo[v]
        size = 8 * wide_y
        for g in range(groups):
            here = slice(g * size, (g + 1) * size)
            blurred = dot3((ext_hi[here, :], ext_lo[here, :]), band)
            lined[8 * g : 8 * g + 8] = dot3(gath, split(blurred)).reshape(8, cols, lanes)
        blur = taps_ref[v, 0, 0] * lined[0:rows]
        for k in range(1, length):
            blur = blur + taps_ref[v, 0, k] * lined[k : k + rows]
        spread[...] = obs[v] / blur
        for g in range(groups):
            pieces = []
            for e in range(8 * g, 8 * g + 8):
                piece = None
                for a in range(rows):
                    if 0 <= e - a < length:
                        term = taps_ref[v, 0, e - a] * spread[a]
                        piece = term if piece is None else piece + term
                pieces.append(piece)
            piece = jnp.concatenate(pieces, axis=0)
            piece = dot3(scat, split(piece))
            piece = dot3(split(piece), band, ((1,), (1,))).reshape(8, wide_y, 2 * lanes)
            dx = 0 if 8 * g < rad else (1 if 8 * g < rad + rows else 2)
            piece = piece * scale[v, dx][None]
            total[8 * g : 8 * g + 8] += piece[:, :, :lanes]
            fringe[8 * g : 8 * g + 8] += piece[:, :, lanes:]
        return carry

    lax.fori_loop(0, views, one_view, 0)

    for g in range(groups):
        merged = fringe[8 * g]
        for i in range(1, 8):
            merged = merged + pltpu.roll(fringe[8 * g + i], 2 * rad * i, 1)
        back_pack[g] = merged
    start(back_z_copies)
    arrive(back_z_copies)
    for g in range(groups):
        merged = jnp.where(lane % (2 * rad) < rad, back_right[g], back_left[g])
        for i in range(8):
            rolled = pltpu.roll(merged, lanes - (2 * rad * i + rad), 1)
            total[8 * g + i] += jnp.where((lane < rad) | (lane >= lanes - rad), rolled, 0.0)
    start(back_xy_copies)
    arrive(back_xy_copies)
    near = back_xy[...]

    def fold(values, size, axis):
        low = lax.slice_in_dim(values, 0, rad, axis=axis)
        mid = lax.slice_in_dim(values, rad, rad + size, axis=axis)
        top = lax.slice_in_dim(values, rad + size, 2 * rad + size, axis=axis)
        if size == 2 * rad:
            return mid + jnp.concatenate([low, top], axis=axis)
        gap_shape = list(low.shape)
        gap_shape[axis] = size - rad
        gap = jnp.zeros(gap_shape, F32)
        return mid + jnp.concatenate([low, gap], axis=axis) + jnp.concatenate([gap, top], axis=axis)

    near = fold(fold(near, rows, 0), cols, 1)
    summed = total[rad : rad + rows, rad : rad + cols, :] + near
    updated = est_ref[...] * (summed / count.reshape(1, 1, lanes))
    out_ref[...] = updated
    stat[1] = jnp.sum(updated.reshape(-1, 8, lanes), axis=0)

    def sums_a():
        for slot, (i, j) in enumerate(ring_a):
            yield pltpu.make_async_remote_copy(
                src_ref=stat,
                dst_ref=stat_a.at[slot],
                send_sem=a_send.at[slot],
                recv_sem=a_recv.at[slot],
                device_id=device_a(i, j),
                device_id_type=MESH,
            )

    def sums_b():
        for i in range(1, n_x):
            yield pltpu.make_async_remote_copy(
                src_ref=part_a,
                dst_ref=stat_b.at[i - 1],
                send_sem=b_send.at[i - 1],
                recv_sem=b_recv.at[i - 1],
                device_id=device_b(i),
                device_id_type=MESH,
            )

    for copy in sums_a():
        copy.start()
    for copy in sums_a():
        copy.wait_recv()
    part_a[...] = stat[...] + jnp.sum(stat_a[...], axis=0)
    for copy in sums_b():
        copy.start()
    for copy in sums_b():
        copy.wait_recv()
    everything = part_a[...] + jnp.sum(stat_b[...], axis=0)
    wanted = jnp.sum(jnp.sum(everything[0], axis=0, keepdims=True), axis=1, keepdims=True)
    gotten = jnp.sum(jnp.sum(everything[1], axis=0, keepdims=True), axis=1, keepdims=True)
    factor = jnp.broadcast_to(wanted, (1, lanes)) / jnp.broadcast_to(gotten, (1, lanes))
    out_ref[...] = out_ref[...] * factor.reshape(1, 1, lanes)

    for family in (xy_copies, z_copies, back_z_copies, back_xy_copies):
        leave(family)
    for copy in sums_a():
        copy.wait_send()
    for copy in sums_b():
        copy.wait_send()


def on_device(sizes, estimate, observed, coverage, psf_taps):
    rows, cols, lanes = estimate.shape
    views = observed.shape[0]
    rad = (psf_taps.shape[2] - 1) // 2
    wide_x, wide_y = rows + 2 * rad, cols + 2 * rad
    groups = wide_x // 8
    n_x, n_y, n_z = sizes
    n_a, n_b = n_y * n_z - 1, n_x - 1

    def vm(*shape, dtype=F32):
        return pltpu.VMEM(shape, dtype)

    def dma(*shape):
        return pltpu.SemaphoreType.DMA(shape)

    scratch = [
        vm(*observed.shape),
        vm(wide_x, wide_y, lanes),
        vm(wide_x * wide_y, 2 * lanes, dtype=BF16),
        vm(wide_x * wide_y, 2 * lanes, dtype=BF16),
        vm(groups, wide_y, lanes),
        vm(groups, wide_y, lanes),
        vm(groups, wide_y, lanes),
        vm(views, lanes),
        vm(3, 3, views, lanes),
        vm(3, 3, views, lanes),
        vm(3, 3, views, lanes),
        vm(views, 3, wide_y, 2 * lanes),
        vm(views, 2 * lanes, lanes, dtype=BF16),
        vm(views, 2 * lanes, lanes, dtype=BF16),
        vm(views, 8 * cols, 8 * wide_y, dtype=BF16),
        vm(views, 8 * cols, 8 * wide_y, dtype=BF16),
        vm(views, 8 * wide_y, 8 * cols, dtype=BF16),
        vm(views, 8 * wide_y, 8 * cols, dtype=BF16),
        vm(wide_x, cols, lanes),
        vm(rows, cols, lanes),
        vm(wide_x, wide_y, lanes),
        vm(wide_x, wide_y, lanes),
        vm(groups, wide_y, lanes),
        vm(groups, wide_y, lanes),
        vm(groups, wide_y, lanes),
        vm(wide_x, wide_y, lanes),
        vm(2, 8, lanes),
        vm(n_a, 2, 8, lanes),
        vm(n_b, 2, 8, lanes),
        vm(2, 8, lanes),
        pltpu.SemaphoreType.DMA,
        dma(8),
        dma(8),
        dma(8),
        dma(8),
        dma(2, 2),
        dma(2, 2),
        dma(2),
        dma(2),
        dma(8),
        dma(8),
        dma(n_a),
        dma(n_a),
        dma(n_b),
        dma(n_b),
    ]
    return pl.pallas_call(
        functools.partial(kernel, sizes),
        out_shape=jax.ShapeDtypeStruct(estimate.shape, F32),
        in_specs=[
            pl.BlockSpec(memory_space=pltpu.SMEM),
            pl.BlockSpec(memory_space=pltpu.SMEM),
            pl.BlockSpec(memory_space=pltpu.VMEM),
            pl.BlockSpec(memory_space=pl.ANY),
        ],
        out_specs=pl.BlockSpec(memory_space=pltpu.VMEM),
        scratch_shapes=scratch,
        compiler_params=pltpu.CompilerParams(collective_id=0, has_side_effects=True),
    )(psf_taps, coverage.reshape(views), estimate, observed)


def solution(mesh):
    sizes = tuple(mesh.shape[axis] for axis in ("bx", "by", "bz"))
    return jax.shard_map(
        functools.partial(on_device, sizes),
        mesh=mesh,
        in_specs=(P("bx", "by", "bz"), P(None, "bx", "by", "bz"), P(None, "bx", "by", "bz"), P()),
        out_specs=P("bx", "by", "bz"),
        check_vma=False,
    )
```

```python
import functools

import jax
import jax.numpy as jnp
from jax import lax
from jax.experimental import pallas as pl
from jax.experimental.pallas import tpu as pltpu
from jax.sharding import PartitionSpec as P

F32 = jnp.float32
BF16 = jnp.bfloat16
MESH = pl.DeviceIdType.MESH


def split(values):
    high = values.astype(BF16)
    low = (values - high.astype(F32)).astype(BF16)
    return high, low


def dot(left, right, dims=((1,), (0,))):
    return lax.dot_general(left, right, (dims, ((), ())), preferred_element_type=F32)


def folded(values):
    half = values.shape[1] // 2
    return values[:, :half] + values[:, half:]


def rings(sizes):
    offsets = [(i, j, k) for i in range(sizes[0]) for j in range(sizes[1]) for k in range(sizes[2])]
    offsets = offsets[1:]
    if len(offsets) < 64:
        return offsets, offsets, []
    return (
        offsets,
        [offset for offset in offsets if offset[0] == 0],
        [offset for offset in offsets if offset[1:] == (0, 0)],
    )


def kernel(
    sizes,
    taps_ref,
    cover_ref,
    est_ref,
    obs_hbm,
    out_ref,
    obs,
    ext,
    ext_hi,
    ext_lo,
    pack,
    from_left,
    from_right,
    weight,
    weight_xy,
    weight_left,
    weight_right,
    scale,
    band,
    twin,
    gath_hi,
    gath_lo,
    scat,
    lined,
    spread,
    total,
    fringe,
    back_pack,
    back_left,
    back_right,
    back_xy,
    stat,
    stat_a,
    stat_b,
    part_a,
    obs_sem,
    out_send,
    out_recv,
    back_send,
    back_recv,
    a_send,
    a_recv,
    b_send,
    b_recv,
):
    n_x, n_y, n_z = sizes
    views, rows, cols, lanes = obs.shape
    length = taps_ref.shape[2]
    rad = (length - 1) // 2
    wide_x, wide_y = rows + 2 * rad, cols + 2 * rad
    groups = wide_x // 8
    me_x, me_y, me_z = lax.axis_index("bx"), lax.axis_index("by"), lax.axis_index("bz")

    fetch = pltpu.make_async_copy(obs_hbm, obs, obs_sem)
    fetch.start()

    def exists(dx, dy, dz):
        ok = None
        for step, me, count in ((dx, me_x, n_x), (dy, me_y, n_y), (dz, me_z, n_z)):
            if step == 0:
                continue
            inside = (me + step >= 0) & (me + step < count)
            ok = inside if ok is None else ok & inside
        return ok

    def device(dx, dy, dz):
        return {"bx": me_x + dx, "by": me_y + dy, "bz": me_z + dz}

    steps = (-1, 0, 1)
    around = [(dx, dy, dz) for dz in steps for dx in steps for dy in steps if (dx, dy, dz) != (0, 0, 0)]
    ring_all, ring_a, ring_b = rings(sizes)

    def partner(i, j, k):
        return {
            "bx": lax.rem(me_x + i, n_x),
            "by": lax.rem(me_y + j, n_y),
            "bz": lax.rem(me_z + k, n_z),
        }

    ext[...] = jnp.zeros(ext.shape, F32)
    ext[rad : rad + rows, rad : rad + cols, :] = est_ref[...]
    from_left[...] = jnp.zeros(from_left.shape, F32)
    from_right[...] = jnp.zeros(from_right.shape, F32)
    weight_xy[...] = jnp.zeros(weight_xy.shape, F32)
    weight_left[...] = jnp.zeros(weight_left.shape, F32)
    weight_right[...] = jnp.zeros(weight_right.shape, F32)
    back_xy[...] = jnp.zeros(back_xy.shape, F32)
    back_left[...] = jnp.zeros(back_left.shape, F32)
    back_right[...] = jnp.zeros(back_right.shape, F32)
    for v in range(views):
        row = jnp.full((1, lanes), cover_ref[v], jnp.int32).astype(F32)
        weight[v : v + 1, :] = row
        weight_xy[1, 1, v : v + 1, :] = row

    barrier = pltpu.get_barrier_semaphore()
    for offset in ring_all:
        pl.semaphore_signal(barrier, inc=1, device_id=partner(*offset), device_id_type=MESH)

    lane = lax.broadcasted_iota(jnp.int32, (cols, lanes), 1)
    for g in range(rows // 8):
        merged = jnp.zeros((cols, lanes), F32)
        for i in range(8):
            rolled = pltpu.roll(est_ref[8 * g + i], 2 * rad * i + rad, 1)
            merged = jnp.where(lane // (2 * rad) == i, rolled, merged)
        pack[g] = merged

    def cut(step, size, width):
        return pl.ds(0, size) if step == 0 else pl.ds(0 if step < 0 else size - width, width)

    def wide(step, size, width):
        return pl.ds(width, size) if step == 0 else pl.ds(0 if step < 0 else width + size, width)

    pack_rows, pack_rad = rows // 8, rad // 8

    def out_copies():
        for slot, (dx, dy, dz) in enumerate(around):
            size, width = (rows, rad) if dz == 0 else (pack_rows, pack_rad)
            source = est_ref if dz == 0 else pack
            target = (from_right, ext, from_left)[dz + 1]
            weights = (weight_right, weight_xy, weight_left)[dz + 1]
            pairs = (
                (
                    source.at[cut(dx, size, width), cut(dy, cols, rad), :],
                    target.at[wide(-dx, size, width), wide(-dy, cols, rad), :],
                ),
                (weight, weights.at[1 - dx, 1 - dy]),
            )
            copies = [
                pltpu.make_async_remote_copy(
                    src_ref=pair[0],
                    dst_ref=pair[1],
                    send_sem=out_send.at[slot, which],
                    recv_sem=out_recv.at[slot, which],
                    device_id=device(dx, dy, dz),
                    device_id_type=MESH,
                )
                for which, pair in enumerate(pairs)
            ]
            yield exists(dx, dy, dz), exists(-dx, -dy, -dz), copies

    def back_copies():
        for slot, (dx, dy, dz) in enumerate(around):
            size, width = (rows, rad) if dz == 0 else (pack_rows, pack_rad)
            source = total if dz == 0 else back_pack
            target = (back_right, back_xy, back_left)[dz + 1]
            copy = pltpu.make_async_remote_copy(
                src_ref=source.at[wide(dx, size, width), wide(dy, cols, rad), :],
                dst_ref=target.at[wide(-dx, size, width), wide(-dy, cols, rad), :],
                send_sem=back_send.at[slot],
                recv_sem=back_recv.at[slot],
                device_id=device(dx, dy, dz),
                device_id_type=MESH,
            )
            yield exists(dx, dy, dz), exists(-dx, -dy, -dz), [copy]

    def start(family):
        for sends, _, copies in family():

            @pl.when(sends)
            def _():
                for copy in copies:
                    copy.start()

    def arrive(family):
        for _, takes, copies in family():

            @pl.when(takes)
            def _():
                for copy in copies:
                    copy.wait_recv()

    def leave(family):
        for sends, _, copies in family():

            @pl.when(sends)
            def _():
                for copy in copies:
                    copy.wait_send()

    def build(v, carry):
        def summed(dim):
            values = [taps_ref[dim, v, k] for k in range(length)]
            while len(values) > 1:
                values = [sum(values[i : i + 2]) for i in range(0, len(values), 2)]
            return jnp.full((8, lanes), values[0], F32)

        inverse = 1.0 / (summed(0) * summed(1) * summed(2))

        def chosen(offset, dim):
            result = jnp.zeros(offset.shape, F32)
            for k in range(length):
                result = jnp.where(offset == k, taps_ref[dim, v, k], result)
            return result

        def iota(shape, dim):
            return lax.broadcasted_iota(jnp.int32, shape, dim)

        shape = (lanes, lanes)
        main = chosen(iota(shape, 0) - iota(shape, 1) + rad, 2)
        shape = (2 * rad, lanes)
        row, col = iota(shape, 0), iota(shape, 1)
        edge = chosen(jnp.where(row < rad, row, row + lanes) - col, 2)
        for first, part in ((0, main), (lanes, edge)):
            part = (part.reshape(-1, 8, lanes) * inverse[None]).reshape(part.shape)
            high, low = split(part)
            band[v, first : first + part.shape[0], :] = jnp.concatenate([high, low], axis=1)
            twin[v, first : first + part.shape[0], :] = jnp.concatenate([high, high], axis=1)
        rest = band.shape[1] - lanes - 2 * rad
        band[v, lanes + 2 * rad :, :] = jnp.zeros((rest, 2 * lanes), BF16)
        twin[v, lanes + 2 * rad :, :] = jnp.zeros((rest, 2 * lanes), BF16)
        shape = (8 * cols, 8 * wide_y)
        row, col = iota(shape, 0), iota(shape, 1)
        offset = jnp.where(row // cols == col // wide_y, col % wide_y - row % cols, -1)
        high, low = split(chosen(offset, 1))
        gath_hi[v], gath_lo[v] = high, low
        shape = (8 * wide_y, 8 * cols)
        row, col = iota(shape, 0), iota(shape, 1)
        offset = jnp.where(row // wide_y == col // cols, row % wide_y - col % cols, -1)
        high, low = split(chosen(offset, 1))
        scat[v] = jnp.concatenate([high, low], axis=1)
        return carry

    early = min(3, views)
    lax.fori_loop(0, early, build, 0)
    pl.semaphore_wait(barrier, len(ring_all))
    start(out_copies)
    lax.fori_loop(early, views, build, 0)

    fetch.wait()
    count = jnp.zeros((1, lanes), F32)
    seen = jnp.zeros((8, lanes), F32)
    for v in range(views):
        count = count + weight[v : v + 1, :]
        seen = seen + weight[v : v + 1, :] * jnp.sum(obs[v].reshape(-1, 8, lanes), axis=0)
    stat[0:1] = jnp.sum(seen / count, axis=0, keepdims=True)

    arrive(out_copies)
    lane = lax.broadcasted_iota(jnp.int32, (wide_y, lanes), 1)
    high, low = split(ext[...].reshape(wide_x * wide_y, lanes))
    ext_hi[:, :lanes] = high
    ext_lo[:, :lanes] = low
    for g in range(groups):
        merged = jnp.where(lane % (2 * rad) < rad, from_left[g], from_right[g])
        for i in range(8):
            shift = (lanes - 2 * rad * i) % lanes
            rolled = pltpu.roll(merged, shift, 1) if shift else merged
            high, low = split(rolled)
            first = (8 * g + i) * wide_y
            ext_hi[first : first + wide_y, lanes:] = high
            ext_lo[first : first + wide_y, lanes:] = low

    thin = lax.broadcasted_iota(jnp.int32, (rad, lanes), 1)
    for v in range(views):
        for dx in range(3):
            for dy in range(3):
                mid = jnp.broadcast_to(weight_xy[dx, dy, v : v + 1, :], (rad, lanes))
                left = jnp.broadcast_to(weight_left[dx, dy, v : v + 1, :], (rad, lanes))
                right = jnp.broadcast_to(weight_right[dx, dy, v : v + 1, :], (rad, lanes))
                side = jnp.where(thin < rad, left, jnp.where(thin < 2 * rad, right, 0.0))
                for first in range(0 if dy == 0 else (rad if dy == 1 else rad + cols), rad if dy == 0 else (rad + cols if dy == 1 else wide_y), rad):
                    scale[v, dx, first : first + rad, :lanes] = mid
                    scale[v, dx, first : first + rad, lanes:] = side

    total[...] = jnp.zeros(total.shape, F32)
    fringe[...] = jnp.zeros(fringe.shape, F32)

    def one_view(v, carry):
        size = 8 * wide_y
        high_part = slice(0, lanes)
        for g in range(groups):
            here = slice(g * size, (g + 1) * size)
            blurred = folded(dot(ext_hi[here, :], band[v])) + dot(ext_lo[here, :], band[v, :, high_part])
            high, low = split(blurred)
            line = folded(dot(gath_hi[v], jnp.concatenate([high, low], axis=1))) + dot(gath_lo[v], high)
            lined[8 * g : 8 * g + 8] = line.reshape(8, cols, lanes)
        blur = taps_ref[0, v, 0] * lined[0:rows]
        for k in range(1, length):
            blur = blur + taps_ref[0, v, k] * lined[k : k + rows]
        spread[...] = obs[v] / blur
        for g in range(groups):
            pieces = []
            for e in range(8 * g, 8 * g + 8):
                piece = None
                for a in range(rows):
                    if 0 <= e - a < length:
                        term = taps_ref[0, v, e - a] * spread[a]
                        piece = term if piece is None else piece + term
                pieces.append(piece)
            piece = jnp.concatenate(pieces, axis=0)
            both = jnp.concatenate(split(piece), axis=1)
            piece = folded(dot(scat[v], jnp.concatenate([both, both], axis=0)))
            high, low = split(piece)
            flip = ((1,), (1,))
            piece = dot(jnp.concatenate([high, low], axis=1), twin[v], flip)
            piece = piece + dot(high, band[v, :, lanes:], flip)
            piece = piece.reshape(8, wide_y, 2 * lanes)
            dx = 0 if 8 * g < rad else (1 if 8 * g < rad + rows else 2)
            piece = piece * scale[v, dx][None]
            total[8 * g : 8 * g + 8] += piece[:, :, :lanes]
            fringe[8 * g : 8 * g + 8] += piece[:, :, lanes:]
        return carry

    lax.fori_loop(0, views, one_view, 0)

    for g in range(groups):
        merged = fringe[8 * g]
        for i in range(1, 8):
            merged = merged + pltpu.roll(fringe[8 * g + i], 2 * rad * i, 1)
        back_pack[g] = merged
    start(back_copies)
    arrive(back_copies)
    near = back_xy[...]

    def fold(values, size, rad, axis):
        low = lax.slice_in_dim(values, 0, rad, axis=axis)
        mid = lax.slice_in_dim(values, rad, rad + size, axis=axis)
        top = lax.slice_in_dim(values, rad + size, 2 * rad + size, axis=axis)
        if size == 2 * rad:
            return mid + jnp.concatenate([low, top], axis=axis)
        gap_shape = list(low.shape)
        gap_shape[axis] = size - rad
        gap = jnp.zeros(gap_shape, F32)
        return mid + jnp.concatenate([low, gap], axis=axis) + jnp.concatenate([gap, top], axis=axis)

    near = fold(fold(near, rows, rad, 0), cols, rad, 1)
    ends = jnp.where((lane % (2 * rad) < rad)[None], back_right[...], back_left[...])
    ends = fold(fold(ends, pack_rows, pack_rad, 0), cols, rad, 1)
    lane = lax.broadcasted_iota(jnp.int32, (cols, lanes), 1)
    outer = (lane < rad) | (lane >= lanes - rad)
    seen = jnp.zeros((8, lanes), F32)
    for x in range(rows):
        rolled = pltpu.roll(ends[x // 8], lanes - (2 * rad * (x % 8) + rad), 1)
        summed = total[rad + x, rad : rad + cols, :] + near[x] + jnp.where(outer, rolled, 0.0)
        updated = est_ref[x] * (summed / count)
        out_ref[x] = updated
        seen = seen + jnp.sum(updated.reshape(-1, 8, lanes), axis=0)
    stat[1:2] = jnp.sum(seen, axis=0, keepdims=True)

    def sums_a():
        for slot, offset in enumerate(ring_a):
            yield pltpu.make_async_remote_copy(
                src_ref=stat,
                dst_ref=stat_a.at[slot],
                send_sem=a_send.at[slot],
                recv_sem=a_recv.at[slot],
                device_id=partner(*offset),
                device_id_type=MESH,
            )

    def sums_b():
        for slot, offset in enumerate(ring_b):
            yield pltpu.make_async_remote_copy(
                src_ref=part_a,
                dst_ref=stat_b.at[slot],
                send_sem=b_send.at[slot],
                recv_sem=b_recv.at[slot],
                device_id=partner(*offset),
                device_id_type=MESH,
            )

    for copy in sums_a():
        copy.start()
    for copy in sums_a():
        copy.wait_recv()
    everything = stat[...] + jnp.sum(stat_a[...], axis=0)
    if ring_b:
        part_a[...] = everything
        for copy in sums_b():
            copy.start()
        for copy in sums_b():
            copy.wait_recv()
        everything = part_a[...] + jnp.sum(stat_b[...], axis=0)
    wanted = jnp.sum(everything[0:1], axis=1, keepdims=True)
    gotten = jnp.sum(everything[1:2], axis=1, keepdims=True)
    factor = jnp.broadcast_to(wanted, (1, lanes)) / jnp.broadcast_to(gotten, (1, lanes))
    out_ref[...] = out_ref[...] * factor.reshape(1, 1, lanes)

    for family in (out_copies, back_copies):
        leave(family)
    for copy in sums_a():
        copy.wait_send()
    for copy in sums_b():
        copy.wait_send()


def on_device(sizes, estimate, observed, coverage, psf_taps):
    rows, cols, lanes = estimate.shape
    views = observed.shape[0]
    rad = (psf_taps.shape[2] - 1) // 2
    wide_x, wide_y = rows + 2 * rad, cols + 2 * rad
    groups = wide_x // 8
    _, ring_a, ring_b = rings(sizes)
    n_a, n_b = len(ring_a), max(1, len(ring_b))

    def vm(*shape, dtype=F32):
        return pltpu.VMEM(shape, dtype)

    def dma(*shape):
        return pltpu.SemaphoreType.DMA(shape)

    scratch = [
        vm(*observed.shape),
        vm(wide_x, wide_y, lanes),
        vm(wide_x * wide_y, 2 * lanes, dtype=BF16),
        vm(wide_x * wide_y, 2 * lanes, dtype=BF16),
        vm(rows // 8, cols, lanes),
        vm(groups, wide_y, lanes),
        vm(groups, wide_y, lanes),
        vm(views, lanes),
        vm(3, 3, views, lanes),
        vm(3, 3, views, lanes),
        vm(3, 3, views, lanes),
        vm(views, 3, wide_y, 2 * lanes),
        vm(views, 2 * lanes, 2 * lanes, dtype=BF16),
        vm(views, 2 * lanes, 2 * lanes, dtype=BF16),
        vm(views, 8 * cols, 8 * wide_y, dtype=BF16),
        vm(views, 8 * cols, 8 * wide_y, dtype=BF16),
        vm(views, 8 * wide_y, 16 * cols, dtype=BF16),
        vm(wide_x, cols, lanes),
        vm(rows, cols, lanes),
        vm(wide_x, wide_y, lanes),
        vm(wide_x, wide_y, lanes),
        vm(groups, wide_y, lanes),
        vm(groups, wide_y, lanes),
        vm(groups, wide_y, lanes),
        vm(wide_x, wide_y, lanes),
        vm(2, lanes),
        vm(n_a, 2, lanes),
        vm(n_b, 2, lanes),
        vm(2, lanes),
        pltpu.SemaphoreType.DMA,
        dma(26, 2),
        dma(26, 2),
        dma(26),
        dma(26),
        dma(n_a),
        dma(n_a),
        dma(n_b),
        dma(n_b),
    ]
    return pl.pallas_call(
        functools.partial(kernel, sizes),
        out_shape=jax.ShapeDtypeStruct(estimate.shape, F32),
        in_specs=[
            pl.BlockSpec(memory_space=pltpu.SMEM),
            pl.BlockSpec(memory_space=pltpu.SMEM),
            pl.BlockSpec(memory_space=pltpu.VMEM),
            pl.BlockSpec(memory_space=pl.ANY),
        ],
        out_specs=pl.BlockSpec(memory_space=pltpu.VMEM),
        scratch_shapes=scratch,
        compiler_params=pltpu.CompilerParams(collective_id=0, has_side_effects=True),
    )(jnp.transpose(psf_taps, (1, 0, 2)), coverage.reshape(views), estimate, observed)


def solution(mesh):
    sizes = tuple(mesh.shape[axis] for axis in ("bx", "by", "bz"))
    return jax.shard_map(
        functools.partial(on_device, sizes),
        mesh=mesh,
        in_specs=(P("bx", "by", "bz"), P(None, "bx", "by", "bz"), P(None, "bx", "by", "bz"), P()),
        out_specs=P("bx", "by", "bz"),
        check_vma=False,
    )
```

```python
import functools

import jax
import jax.numpy as jnp
from jax import lax
from jax.experimental import pallas as pl
from jax.experimental.pallas import tpu as pltpu
from jax.sharding import PartitionSpec as P

F32 = jnp.float32
BF16 = jnp.bfloat16
MESH = pl.DeviceIdType.MESH


def split(values):
    high = values.astype(BF16)
    low = (values - high.astype(F32)).astype(BF16)
    return high, low


def dot(left, right, dims=((1,), (0,))):
    return lax.dot_general(left, right, (dims, ((), ())), preferred_element_type=F32)


def folded(values):
    half = values.shape[1] // 2
    return values[:, :half] + values[:, half:]


def rings(sizes):
    offsets = [(i, j, k) for i in range(sizes[0]) for j in range(sizes[1]) for k in range(sizes[2])]
    offsets = offsets[1:]
    if len(offsets) < 64:
        return offsets, offsets, []
    return (
        offsets,
        [offset for offset in offsets if offset[0] == 0],
        [offset for offset in offsets if offset[1:] == (0, 0)],
    )


def kernel(
    sizes,
    taps_ref,
    cover_ref,
    est_ref,
    obs_hbm,
    out_ref,
    obs,
    ext,
    ext_hi,
    ext_lo,
    pack,
    from_left,
    from_right,
    weight,
    weight_xy,
    weight_left,
    weight_right,
    scale,
    band,
    twin,
    gath_hi,
    gath_lo,
    scat,
    lined,
    spread,
    total,
    fringe,
    back_pack,
    back_left,
    back_right,
    back_xy,
    stat,
    stat_a,
    stat_b,
    part_a,
    obs_sem,
    out_send,
    out_recv,
    back_send,
    back_recv,
    a_send,
    a_recv,
    b_send,
    b_recv,
):
    n_x, n_y, n_z = sizes
    views, rows, cols, lanes = obs.shape
    length = taps_ref.shape[2]
    rad = (length - 1) // 2
    wide_x, wide_y = rows + 2 * rad, cols + 2 * rad
    groups = wide_x // 8
    me_x, me_y, me_z = lax.axis_index("bx"), lax.axis_index("by"), lax.axis_index("bz")

    fetch = pltpu.make_async_copy(obs_hbm, obs, obs_sem)
    fetch.start()

    def exists(dx, dy, dz):
        ok = None
        for step, me, count in ((dx, me_x, n_x), (dy, me_y, n_y), (dz, me_z, n_z)):
            if step == 0:
                continue
            inside = (me + step >= 0) & (me + step < count)
            ok = inside if ok is None else ok & inside
        return ok

    def device(dx, dy, dz):
        return {"bx": me_x + dx, "by": me_y + dy, "bz": me_z + dz}

    steps = (-1, 0, 1)
    around = [(dx, dy, dz) for dz in steps for dx in steps for dy in steps if (dx, dy, dz) != (0, 0, 0)]
    ring_all, ring_a, ring_b = rings(sizes)

    def partner(i, j, k):
        return {
            "bx": lax.rem(me_x + i, n_x),
            "by": lax.rem(me_y + j, n_y),
            "bz": lax.rem(me_z + k, n_z),
        }

    ext[...] = jnp.zeros(ext.shape, F32)
    ext[rad : rad + rows, rad : rad + cols, :] = est_ref[...]
    from_left[...] = jnp.zeros(from_left.shape, F32)
    from_right[...] = jnp.zeros(from_right.shape, F32)
    weight_xy[...] = jnp.zeros(weight_xy.shape, F32)
    weight_left[...] = jnp.zeros(weight_left.shape, F32)
    weight_right[...] = jnp.zeros(weight_right.shape, F32)
    back_xy[...] = jnp.zeros(back_xy.shape, F32)
    back_left[...] = jnp.zeros(back_left.shape, F32)
    back_right[...] = jnp.zeros(back_right.shape, F32)
    for v in range(views):
        row = jnp.full((1, lanes), cover_ref[v], jnp.int32).astype(F32)
        weight[v : v + 1, :] = row
        weight_xy[1, 1, v : v + 1, :] = row

    barrier = pltpu.get_barrier_semaphore()
    for offset in ring_all:
        pl.semaphore_signal(barrier, inc=1, device_id=partner(*offset), device_id_type=MESH)

    lane = lax.broadcasted_iota(jnp.int32, (cols, lanes), 1)
    for g in range(rows // 8):
        merged = jnp.zeros((cols, lanes), F32)
        for i in range(8):
            rolled = pltpu.roll(est_ref[8 * g + i], 2 * rad * i + rad, 1)
            merged = jnp.where(lane // (2 * rad) == i, rolled, merged)
        pack[g] = merged

    def cut(step, size, width):
        return pl.ds(0, size) if step == 0 else pl.ds(0 if step < 0 else size - width, width)

    def wide(step, size, width):
        return pl.ds(width, size) if step == 0 else pl.ds(0 if step < 0 else width + size, width)

    pack_rows, pack_rad = rows // 8, rad // 8

    def out_copies():
        for slot, (dx, dy, dz) in enumerate(around):
            size, width = (rows, rad) if dz == 0 else (pack_rows, pack_rad)
            source = est_ref if dz == 0 else pack
            target = (from_right, ext, from_left)[dz + 1]
            weights = (weight_right, weight_xy, weight_left)[dz + 1]
            pairs = (
                (
                    source.at[cut(dx, size, width), cut(dy, cols, rad), :],
                    target.at[wide(-dx, size, width), wide(-dy, cols, rad), :],
                ),
                (weight, weights.at[1 - dx, 1 - dy]),
            )
            copies = [
                pltpu.make_async_remote_copy(
                    src_ref=pair[0],
                    dst_ref=pair[1],
                    send_sem=out_send.at[slot, which],
                    recv_sem=out_recv.at[slot, which],
                    device_id=device(dx, dy, dz),
                    device_id_type=MESH,
                )
                for which, pair in enumerate(pairs)
            ]
            yield exists(dx, dy, dz), exists(-dx, -dy, -dz), copies

    def back_copies():
        for slot, (dx, dy, dz) in enumerate(around):
            size, width = (rows, rad) if dz == 0 else (pack_rows, pack_rad)
            source = total if dz == 0 else back_pack
            target = (back_right, back_xy, back_left)[dz + 1]
            copy = pltpu.make_async_remote_copy(
                src_ref=source.at[wide(dx, size, width), wide(dy, cols, rad), :],
                dst_ref=target.at[wide(-dx, size, width), wide(-dy, cols, rad), :],
                send_sem=back_send.at[slot],
                recv_sem=back_recv.at[slot],
                device_id=device(dx, dy, dz),
                device_id_type=MESH,
            )
            yield exists(dx, dy, dz), exists(-dx, -dy, -dz), [copy]

    def start(family):
        for sends, _, copies in family():

            @pl.when(sends)
            def _():
                for copy in copies:
                    copy.start()

    def arrive(family):
        for _, takes, copies in family():

            @pl.when(takes)
            def _():
                for copy in copies:
                    copy.wait_recv()

    def leave(family):
        for sends, _, copies in family():

            @pl.when(sends)
            def _():
                for copy in copies:
                    copy.wait_send()

    def build(v, carry):
        def summed(dim):
            values = [taps_ref[dim, v, k] for k in range(length)]
            while len(values) > 1:
                values = [sum(values[i : i + 2]) for i in range(0, len(values), 2)]
            return jnp.full((8, lanes), values[0], F32)

        inverse = 1.0 / (summed(0) * summed(1) * summed(2))

        def chosen(offset, dim):
            result = jnp.zeros(offset.shape, F32)
            for k in range(length):
                result = jnp.where(offset == k, taps_ref[dim, v, k], result)
            return result

        def iota(shape, dim):
            return lax.broadcasted_iota(jnp.int32, shape, dim)

        shape = (lanes, lanes)
        main = chosen(iota(shape, 0) - iota(shape, 1) + rad, 2)
        shape = (2 * rad, lanes)
        row, col = iota(shape, 0), iota(shape, 1)
        edge = chosen(jnp.where(row < rad, row, row + lanes) - col, 2)
        for first, part in ((0, main), (lanes, edge)):
            part = (part.reshape(-1, 8, lanes) * inverse[None]).reshape(part.shape)
            high, low = split(part)
            band[v, first : first + part.shape[0], :] = jnp.concatenate([high, low], axis=1)
            twin[v, first : first + part.shape[0], :] = jnp.concatenate([high, high], axis=1)
        rest = band.shape[1] - lanes - 2 * rad
        band[v, lanes + 2 * rad :, :] = jnp.zeros((rest, 2 * lanes), BF16)
        twin[v, lanes + 2 * rad :, :] = jnp.zeros((rest, 2 * lanes), BF16)
        shape = (8 * cols, 8 * wide_y)
        row, col = iota(shape, 0), iota(shape, 1)
        offset = jnp.where(row // cols == col // wide_y, col % wide_y - row % cols, -1)
        high, low = split(chosen(offset, 1))
        gath_hi[v], gath_lo[v] = high, low
        shape = (8 * wide_y, 8 * cols)
        row, col = iota(shape, 0), iota(shape, 1)
        offset = jnp.where(row // wide_y == col // cols, row % wide_y - col % cols, -1)
        high, low = split(chosen(offset, 1))
        scat[v] = jnp.concatenate([high, low], axis=1)
        return carry

    early = min(3, views)
    lax.fori_loop(0, early, build, 0)
    pl.semaphore_wait(barrier, len(ring_all))
    start(out_copies)
    lax.fori_loop(early, views, build, 0)

    fetch.wait()
    count = jnp.zeros((1, lanes), F32)
    seen = jnp.zeros((8, lanes), F32)
    for v in range(views):
        count = count + weight[v : v + 1, :]
        seen = seen + weight[v : v + 1, :] * jnp.sum(obs[v].reshape(-1, 8, lanes), axis=0)
    stat[0:1] = jnp.sum(seen / count, axis=0, keepdims=True)

    arrive(out_copies)
    lane = lax.broadcasted_iota(jnp.int32, (wide_y, lanes), 1)
    high, low = split(ext[...].reshape(wide_x * wide_y, lanes))
    ext_hi[:, :lanes] = high
    ext_lo[:, :lanes] = low
    for g in range(groups):
        merged = jnp.where(lane % (2 * rad) < rad, from_left[g], from_right[g])
        for i in range(8):
            shift = (lanes - 2 * rad * i) % lanes
            rolled = pltpu.roll(merged, shift, 1) if shift else merged
            high, low = split(rolled)
            first = (8 * g + i) * wide_y
            ext_hi[first : first + wide_y, lanes:] = high
            ext_lo[first : first + wide_y, lanes:] = low

    thin = lax.broadcasted_iota(jnp.int32, (rad, lanes), 1)
    for v in range(views):
        for dx in range(3):
            for dy in range(3):
                mid = jnp.broadcast_to(weight_xy[dx, dy, v : v + 1, :], (rad, lanes))
                left = jnp.broadcast_to(weight_left[dx, dy, v : v + 1, :], (rad, lanes))
                right = jnp.broadcast_to(weight_right[dx, dy, v : v + 1, :], (rad, lanes))
                side = jnp.where(thin < rad, left, jnp.where(thin < 2 * rad, right, 0.0))
                for first in range(0 if dy == 0 else (rad if dy == 1 else rad + cols), rad if dy == 0 else (rad + cols if dy == 1 else wide_y), rad):
                    scale[v, dx, first : first + rad, :lanes] = mid
                    scale[v, dx, first : first + rad, lanes:] = side

    total[...] = jnp.zeros(total.shape, F32)
    fringe[...] = jnp.zeros(fringe.shape, F32)

    def one_view(v, carry):
        size = 8 * wide_y
        high_part = slice(0, lanes)
        for g in range(groups):
            here = slice(g * size, (g + 1) * size)
            blurred = folded(dot(ext_hi[here, :], band[v])) + dot(ext_lo[here, :], band[v, :, high_part])
            high, low = split(blurred)
            line = folded(dot(gath_hi[v], jnp.concatenate([high, low], axis=1))) + dot(gath_lo[v], high)
            lined[8 * g : 8 * g + 8] = line.reshape(8, cols, lanes)
        blur = taps_ref[0, v, 0] * lined[0:rows]
        for k in range(1, length):
            blur = blur + taps_ref[0, v, k] * lined[k : k + rows]
        spread[...] = obs[v] / blur
        for g in range(groups):
            pieces = []
            for e in range(8 * g, 8 * g + 8):
                piece = None
                for a in range(rows):
                    if 0 <= e - a < length:
                        term = taps_ref[0, v, e - a] * spread[a]
                        piece = term if piece is None else piece + term
                pieces.append(piece)
            piece = jnp.concatenate(pieces, axis=0)
            both = jnp.concatenate(split(piece), axis=1)
            piece = folded(dot(scat[v], jnp.concatenate([both, both], axis=0)))
            high, low = split(piece)
            flip = ((1,), (1,))
            piece = dot(jnp.concatenate([high, low], axis=1), twin[v], flip)
            piece = piece + dot(high, band[v, :, lanes:], flip)
            piece = piece.reshape(8, wide_y, 2 * lanes)
            dx = 0 if 8 * g < rad else (1 if 8 * g < rad + rows else 2)
            piece = piece * scale[v, dx][None]
            total[8 * g : 8 * g + 8] += piece[:, :, :lanes]
            fringe[8 * g : 8 * g + 8] += piece[:, :, lanes:]
        return carry

    lax.fori_loop(0, views, one_view, 0, unroll=2)

    for g in range(groups):
        merged = fringe[8 * g]
        for i in range(1, 8):
            merged = merged + pltpu.roll(fringe[8 * g + i], 2 * rad * i, 1)
        back_pack[g] = merged
    start(back_copies)
    arrive(back_copies)
    near = back_xy[...]

    def fold(values, size, rad, axis):
        low = lax.slice_in_dim(values, 0, rad, axis=axis)
        mid = lax.slice_in_dim(values, rad, rad + size, axis=axis)
        top = lax.slice_in_dim(values, rad + size, 2 * rad + size, axis=axis)
        if size == 2 * rad:
            return mid + jnp.concatenate([low, top], axis=axis)
        gap_shape = list(low.shape)
        gap_shape[axis] = size - rad
        gap = jnp.zeros(gap_shape, F32)
        return mid + jnp.concatenate([low, gap], axis=axis) + jnp.concatenate([gap, top], axis=axis)

    near = fold(fold(near, rows, rad, 0), cols, rad, 1)
    ends = jnp.where((lane % (2 * rad) < rad)[None], back_right[...], back_left[...])
    ends = fold(fold(ends, pack_rows, pack_rad, 0), cols, rad, 1)
    lane = lax.broadcasted_iota(jnp.int32, (cols, lanes), 1)
    outer = (lane < rad) | (lane >= lanes - rad)
    seen = jnp.zeros((8, lanes), F32)
    for x in range(rows):
        rolled = pltpu.roll(ends[x // 8], lanes - (2 * rad * (x % 8) + rad), 1)
        summed = total[rad + x, rad : rad + cols, :] + near[x] + jnp.where(outer, rolled, 0.0)
        updated = est_ref[x] * (summed / count)
        out_ref[x] = updated
        seen = seen + jnp.sum(updated.reshape(-1, 8, lanes), axis=0)
    stat[1:2] = jnp.sum(seen, axis=0, keepdims=True)

    def sums_a():
        for slot, offset in enumerate(ring_a):
            yield pltpu.make_async_remote_copy(
                src_ref=stat,
                dst_ref=stat_a.at[slot],
                send_sem=a_send.at[slot],
                recv_sem=a_recv.at[slot],
                device_id=partner(*offset),
                device_id_type=MESH,
            )

    def sums_b():
        for slot, offset in enumerate(ring_b):
            yield pltpu.make_async_remote_copy(
                src_ref=part_a,
                dst_ref=stat_b.at[slot],
                send_sem=b_send.at[slot],
                recv_sem=b_recv.at[slot],
                device_id=partner(*offset),
                device_id_type=MESH,
            )

    for copy in sums_a():
        copy.start()
    for copy in sums_a():
        copy.wait_recv()
    everything = stat[...] + jnp.sum(stat_a[...], axis=0)
    if ring_b:
        part_a[...] = everything
        for copy in sums_b():
            copy.start()
        for copy in sums_b():
            copy.wait_recv()
        everything = part_a[...] + jnp.sum(stat_b[...], axis=0)
    wanted = jnp.sum(everything[0:1], axis=1, keepdims=True)
    gotten = jnp.sum(everything[1:2], axis=1, keepdims=True)
    factor = jnp.broadcast_to(wanted, (1, lanes)) / jnp.broadcast_to(gotten, (1, lanes))
    out_ref[...] = out_ref[...] * factor.reshape(1, 1, lanes)

    for family in (out_copies, back_copies):
        leave(family)
    for copy in sums_a():
        copy.wait_send()
    for copy in sums_b():
        copy.wait_send()


def on_device(sizes, estimate, observed, coverage, psf_taps):
    rows, cols, lanes = estimate.shape
    views = observed.shape[0]
    rad = (psf_taps.shape[2] - 1) // 2
    wide_x, wide_y = rows + 2 * rad, cols + 2 * rad
    groups = wide_x // 8
    _, ring_a, ring_b = rings(sizes)
    n_a, n_b = len(ring_a), max(1, len(ring_b))

    def vm(*shape, dtype=F32):
        return pltpu.VMEM(shape, dtype)

    def dma(*shape):
        return pltpu.SemaphoreType.DMA(shape)

    scratch = [
        vm(*observed.shape),
        vm(wide_x, wide_y, lanes),
        vm(wide_x * wide_y, 2 * lanes, dtype=BF16),
        vm(wide_x * wide_y, 2 * lanes, dtype=BF16),
        vm(rows // 8, cols, lanes),
        vm(groups, wide_y, lanes),
        vm(groups, wide_y, lanes),
        vm(views, lanes),
        vm(3, 3, views, lanes),
        vm(3, 3, views, lanes),
        vm(3, 3, views, lanes),
        vm(views, 3, wide_y, 2 * lanes),
        vm(views, 2 * lanes, 2 * lanes, dtype=BF16),
        vm(views, 2 * lanes, 2 * lanes, dtype=BF16),
        vm(views, 8 * cols, 8 * wide_y, dtype=BF16),
        vm(views, 8 * cols, 8 * wide_y, dtype=BF16),
        vm(views, 8 * wide_y, 16 * cols, dtype=BF16),
        vm(wide_x, cols, lanes),
        vm(rows, cols, lanes),
        vm(wide_x, wide_y, lanes),
        vm(wide_x, wide_y, lanes),
        vm(groups, wide_y, lanes),
        vm(groups, wide_y, lanes),
        vm(groups, wide_y, lanes),
        vm(wide_x, wide_y, lanes),
        vm(2, lanes),
        vm(n_a, 2, lanes),
        vm(n_b, 2, lanes),
        vm(2, lanes),
        pltpu.SemaphoreType.DMA,
        dma(26, 2),
        dma(26, 2),
        dma(26),
        dma(26),
        dma(n_a),
        dma(n_a),
        dma(n_b),
        dma(n_b),
    ]
    return pl.pallas_call(
        functools.partial(kernel, sizes),
        out_shape=jax.ShapeDtypeStruct(estimate.shape, F32),
        in_specs=[
            pl.BlockSpec(memory_space=pltpu.SMEM),
            pl.BlockSpec(memory_space=pltpu.SMEM),
            pl.BlockSpec(memory_space=pltpu.VMEM),
            pl.BlockSpec(memory_space=pl.ANY),
        ],
        out_specs=pl.BlockSpec(memory_space=pltpu.VMEM),
        scratch_shapes=scratch,
        compiler_params=pltpu.CompilerParams(collective_id=0, has_side_effects=True),
    )(jnp.transpose(psf_taps, (1, 0, 2)), coverage.reshape(views), estimate, observed)


def solution(mesh):
    sizes = tuple(mesh.shape[axis] for axis in ("bx", "by", "bz"))
    return jax.shard_map(
        functools.partial(on_device, sizes),
        mesh=mesh,
        in_specs=(P("bx", "by", "bz"), P(None, "bx", "by", "bz"), P(None, "bx", "by", "bz"), P()),
        out_specs=P("bx", "by", "bz"),
        check_vma=False,
    )
```
